32 devices in a mesh: m: 2 (over x), kk: 4 (over z), g: 4 (over y, core).
Axes of the slice: x: 2, y: 2, z: 4, core: 2. Of those that a mesh axis runs over, the one named last changes fastest.
Arguments:
- a_mat: bfloat16 [16384, 28672], P(('m', 'g'), 'kk'), parts along dimension 0
Outputs:
- output: float32 [8, 3, 2048, 2048], P(('m', 'g'), None, 'kk'), parts along dimension 0
There are 2 independent parts. The reference program is written for one: setup_inputs(seed, part) draws one part's arguments, and reference() takes and returns one part's arrays. A program takes and returns all parts, laid end to end along the dimension named above; each array names one.
All inputs are finite; a program needn't handle non-finite values.
Results may differ from the reference program's by a relative error of at most 0.001.
Values are sent between devices in bfloat16 or wider.
A program may use at most 1 GiB of HBM per device.

```python
import math
import jax
import jax.numpy as jnp
from jax import lax

N_ROWS = 8192
K_COLS = 28672
GROUP_SIZE = 4

BLOCK_ROWS = N_ROWS // GROUP_SIZE
SLOT_COUNT = GROUP_SIZE // 2 + 1


def pair_table(groups):
    half_size = groups // 2
    step_width = max(1, math.isqrt(half_size))
    left_tab = []
    right_tab = []
    for dev_pos in range(groups):
        left_tab.append(dev_pos)
        right_tab.append(dev_pos)
        for diff_pos in range(1, half_size + 1):
            big_off = -(-diff_pos // step_width) * step_width
            if 2 * diff_pos == groups and dev_pos >= half_size:
                left_tab.append(-1)
                right_tab.append(-1)
            else:
                left_tab.append((dev_pos + big_off) % groups)
                right_tab.append((dev_pos + big_off - diff_pos) % groups)
    return left_tab, right_tab


def setup_inputs(seed: int = 0, part: int = 0) -> dict:
    base_key = jax.random.fold_in(jax.random.key(seed), part)
    key_val, key_scale = jax.random.split(base_key)
    values = jax.random.normal(key_val, (GROUP_SIZE, BLOCK_ROWS, K_COLS), jnp.float32)
    block_scale = jax.random.uniform(key_scale, (GROUP_SIZE, 1, 1), jnp.float32, 0.7, 1.4)
    a_mat = (values * block_scale).reshape(N_ROWS, K_COLS) * (K_COLS ** -0.25)
    return {"a_mat": a_mat.astype(jnp.bfloat16)}


def reference(a_mat):
    left_tab, right_tab = pair_table(GROUP_SIZE)
    pair_idx = jnp.array([[max(left_val, 0), max(right_val, 0)] for left_val, right_val in zip(left_tab, right_tab)], dtype=jnp.int32)
    keep_slot = jnp.array([left_val >= 0 for left_val in left_tab])
    blocks = a_mat.reshape(GROUP_SIZE, BLOCK_ROWS, K_COLS)

    def one_block(pair_row):
        row_blk = lax.dynamic_index_in_dim(blocks, pair_row[0], 0, keepdims=False)
        col_blk = lax.dynamic_index_in_dim(blocks, pair_row[1], 0, keepdims=False)
        return jnp.dot(row_blk, col_blk.T, preferred_element_type=jnp.float32)

    products = lax.map(one_block, pair_idx)
    products = jnp.where(keep_slot[:, None, None], products, 0.0)
    return products.reshape(GROUP_SIZE, SLOT_COUNT, BLOCK_ROWS, BLOCK_ROWS)
```

```python
import jax
import jax.numpy as jnp
from jax import lax
from jax.experimental import pallas as pl
from jax.experimental.pallas import tpu as pltpu
from jax.sharding import PartitionSpec as P


PIECES = ((1, 3), (2,), (1,), (1,))
CHIP_SWAP = [(0, 1), (1, 0), (2, 3), (3, 2)]
CROSS = [(0, 3), (1, 2), (2, 0), (3, 1)]
DEPTH = 3584
VMEM = 60 * 1024 * 1024
ANY = pl.BlockSpec(memory_space=pl.ANY)


def dot_t(left, right):
    return lax.dot_general(left, right, (((1,), (1,)), ((), ())), preferred_element_type=jnp.float32)


def mm(load_l, load_r, cols, acc):
    acc[...] = jnp.zeros_like(acc)

    def step(k, _):
        ks = pl.ds(pl.multiple_of(k * DEPTH, DEPTH), DEPTH)
        acc[...] += dot_t(load_l(ks), load_r(ks))
        return 0

    lax.fori_loop(0, cols // DEPTH, step, 0)


def cost(m, n, k):
    return pl.CostEstimate(flops=2 * m * n * k, bytes_accessed=2 * (m + n) * k + 4 * m * n, transcendentals=0)


def params(n):
    return pltpu.CompilerParams(vmem_limit_bytes=VMEM, dimension_semantics=("arbitrary",) * n)


def same_call(a, zs):
    rows, cols = a.shape
    q = rows // zs

    def body(a_ref, o_ref):
        mm(lambda ks: a_ref[:, ks], lambda ks: a_ref[:, ks], cols, o_ref.at[0])

    return pl.pallas_call(
        body,
        grid=(zs,),
        in_specs=[pl.BlockSpec((q, cols), lambda r: (r, 0))],
        out_specs=pl.BlockSpec((1, q, q), lambda r: (r, 0, 0)),
        out_shape=jax.ShapeDtypeStruct((zs, q, q), jnp.float32),
        compiler_params=params(1),
        cost_estimate=cost(rows, q, cols),
        name="same_block",
    )(a)


def rest_call(a, dep, zs):
    rows, cols = a.shape
    q = rows // zs
    h = q // 2

    def body(l_ref, r_ref, dep_ref, o_ref):
        mm(lambda ks: l_ref[:, ks], lambda ks: r_ref[:, ks], cols, o_ref.at[0])

    def left(r, c):
        return (jnp.where((c == 2) & (r >= 2), r - 2, r), 0)

    def right(r, c):
        far = jnp.where(r < 2, 2 * (r + 2), 2 * r + 1)
        return (jnp.where(c == 2, far, 2 * ((r + 3) % 4) + c), 0)

    return pl.pallas_call(
        body,
        grid=(zs, 3),
        in_specs=[pl.BlockSpec((q, cols), left), pl.BlockSpec((h, cols), right), ANY],
        out_specs=pl.BlockSpec((1, q, h), lambda r, c: (r, 0, c)),
        out_shape=jax.ShapeDtypeStruct((zs, q, 3 * h), jnp.float32),
        compiler_params=params(2),
        cost_estimate=cost(rows, 3 * h, cols),
        name="rest_block",
    )(a, a, dep)


def near_call(left, right, which, dep, zs):
    rows, cols = left.shape
    h = rows // zs // 2

    def body(l_ref, r_ref, dep_ref, o_ref):
        mm(lambda ks: l_ref[:, 0, :, ks].reshape(zs * h, -1), lambda ks: r_ref[:, ks], cols, o_ref)

    return pl.pallas_call(
        body,
        grid=(rows // h,),
        in_specs=[
            pl.BlockSpec((zs, 1, h, cols), lambda j: (0, which, 0, 0), pipeline_mode=pl.Buffered(1)),
            pl.BlockSpec((h, cols), lambda j: (j, 0)),
            ANY,
        ],
        out_specs=pl.BlockSpec((zs * h, h), lambda j: (0, j)),
        out_shape=jax.ShapeDtypeStruct((zs * h, rows), jnp.float32),
        compiler_params=params(1),
        cost_estimate=cost(zs * h, rows, cols),
        name="near_block",
    )(left.reshape(zs, 2, h, cols), right, dep)


def cross_call(pos, gots, a, dep, zs):
    rows, cols = a.shape
    q = rows // zs
    sizes = [x.shape[0] // zs for x in gots]
    n = sum(sizes)

    def body(pos_ref, *refs):
        l_refs, (r_ref, dep_ref, o_ref, acc) = refs[: len(sizes)], refs[len(sizes) :]
        j = pl.program_id(0)
        lo = 0
        for l_ref, size in zip(l_refs, sizes):
            part = acc.at[:, : zs * size]
            mm(lambda ks: r_ref[:, ks], lambda ks: l_ref[:, ks], cols, part)

            @pl.when(pos_ref[0] != 2)
            def _():
                prod = part[...].T
                for s in range(zs):
                    o_ref[s, lo : lo + size, pl.ds(pl.multiple_of(j * q, q), q)] = prod[s * size : (s + 1) * size]

            @pl.when(pos_ref[0] == 2)
            def _():
                prod = part[...].T
                for s in range(zs):
                    o_ref[j, lo : lo + size, s * q : (s + 1) * q] = prod[s * size : (s + 1) * size]

            lo += size

    return pl.pallas_call(
        body,
        grid_spec=pltpu.PrefetchScalarGridSpec(
            num_scalar_prefetch=1,
            grid=(zs,),
            in_specs=[pl.BlockSpec(x.shape, lambda j, p: (0, 0), pipeline_mode=pl.Buffered(1)) for x in gots]
            + [pl.BlockSpec((q, cols), lambda j, p: (j, 0)), ANY],
            out_specs=pl.BlockSpec((zs, n, rows), lambda j, p: (0, 0, 0)),
            scratch_shapes=[pltpu.VMEM((q, zs * max(sizes)), jnp.float32)],
        ),
        out_shape=jax.ShapeDtypeStruct((zs, n, rows), jnp.float32),
        compiler_params=params(1),
        cost_estimate=cost(zs * n, rows, cols),
        name="cross_block",
    )(pos, *gots, a, dep)


def own_call(zpos, same, low, up, far, far_other, rows):
    q = same.shape[0]

    def body(z_ref, same_ref, low_ref, up_ref, far_ref, other_ref, o_ref):
        z = z_ref[0]

        def cols(rel):
            return pl.ds(pl.multiple_of(((z + rel) % 4) * q, q), q)

        o_ref[0, :, cols(0)] = same_ref[...]
        o_ref[0, :, cols(1)] = up_ref[...].T
        o_ref[0, :, cols(3)] = low_ref[...]

        @pl.when(z < 2)
        def _():
            o_ref[0, :, cols(2)] = jnp.concatenate([far_ref[...], other_ref[...]], axis=1)

        @pl.when(z >= 2)
        def _():
            o_ref[0, :, cols(2)] = jnp.concatenate([other_ref[...], far_ref[...]], axis=1).T

    whole = lambda x: pl.BlockSpec(x.shape, lambda i, z: (0, 0))
    ins = (same, low, up, far, far_other)
    return pl.pallas_call(
        body,
        grid_spec=pltpu.PrefetchScalarGridSpec(
            num_scalar_prefetch=1,
            grid=(1,),
            in_specs=[whole(x) for x in ins],
            out_specs=pl.BlockSpec((1, q, rows), lambda i, z: (0, 0, 0)),
        ),
        out_shape=jax.ShapeDtypeStruct((3, q, rows), jnp.float32),
        compiler_params=params(1),
        name="own_out",
    )(zpos, *ins)


def slots_call(pos, out, near, near_other, mine, sent):
    _, q, rows = out.shape
    spans = []
    for x in mine:
        lo = spans[-1][1] if spans else 0
        spans.append((lo, lo + x.shape[0]))
    n = len(mine)

    def body(p_ref, out_ref, near_ref, other_ref, *refs):
        mine_refs, sent_refs, o_ref, buf = refs[:n], refs[n : 2 * n], refs[2 * n], refs[2 * n + 1]
        p = p_ref[0]
        slot = pl.program_id(0) + 1

        @pl.when(((slot == 1) & (p == 3)) | ((slot == 2) & (p < 2)))
        def _():
            for (lo, hi), ref in zip(spans, mine_refs):
                o_ref[0, lo:hi, :] = ref[...]

        @pl.when((slot == 2) & (p >= 2))
        def _():
            o_ref[...] = jnp.zeros_like(o_ref)

        @pl.when((slot == 1) & (p % 2 == 0))
        def _():
            o_ref[0, : q // 2, :] = near_ref[...]
            o_ref[0, q // 2 :, :] = other_ref[...]

        @pl.when((slot == 1) & (p == 1))
        def _():
            for (lo, hi), ref in zip(spans, sent_refs):
                buf[lo:hi, :] = ref[...]
            for s in range(rows // q):
                o_ref[0, :, s * q : (s + 1) * q] = buf[:, s * q : (s + 1) * q].T

    whole = lambda x: pl.BlockSpec(x.shape, lambda i, p: (0, 0), pipeline_mode=pl.Buffered(1))
    ins = (near, near_other, *mine, *sent)
    return pl.pallas_call(
        body,
        grid_spec=pltpu.PrefetchScalarGridSpec(
            num_scalar_prefetch=1,
            grid=(2,),
            in_specs=[ANY] + [whole(x) for x in ins],
            out_specs=pl.BlockSpec((1, q, rows), lambda i, p: (i + 1, 0, 0)),
            scratch_shapes=[pltpu.VMEM((q, rows), jnp.float32)],
        ),
        out_shape=jax.ShapeDtypeStruct(out.shape, jnp.float32),
        input_output_aliases={1: 0},
        compiler_params=params(1),
        name="slots_out",
    )(pos, out, *ins)


def solution(mesh):
    assert mesh.shape["g"] == 4 and mesh.shape["kk"] == 4
    zs = 4

    def scatter(parts):
        return lax.psum_scatter(parts, "kk", scatter_dimension=0, tiled=False)

    def local_fn(a):
        pos = lax.axis_index("g").astype(jnp.int32)
        zpos = lax.axis_index("kk").astype(jnp.int32)
        pos1, zpos1 = pos.reshape(1), zpos.reshape(1)
        rows, cols = a.shape
        q = rows // zs
        h = q // 2
        a4 = a.reshape(zs, q, cols)
        unit = q // sum(map(sum, PIECES))

        arrived, start, gives = [], 0, 0
        for sizes in PIECES:
            arrived.append([])
            for n in sizes:
                piece = a4[:, start : start + n * unit].reshape(-1, cols)
                arrived[-1].append(lax.ppermute(piece, "g", CROSS))
                start += n * unit
                gives += 1
        partner = lax.ppermute(a, "g", CHIP_SWAP)

        same_part = same_call(a, zs)
        same = scatter(same_part)
        rest_part = rest_call(a, same_part, zs)
        rest = scatter(rest_part)

        even = pos % 2 == 0
        near_part = lax.cond(
            even,
            lambda: near_call(partner, a, 0, rest_part, zs),
            lambda: near_call(a, partner, 1, rest_part, zs),
        )
        near = scatter(near_part.reshape(zs, h, rows))

        mine, sent, dep = [], [], near_part
        for got in arrived:
            dep = cross_call(pos1, got, a, dep, zs)
            mine.append(scatter(dep))

        low, far = rest[:, :q], rest[:, q:]
        up = lax.ppermute(low, "kk", [(r, (r - 1) % zs) for r in range(zs)])
        far_other = lax.ppermute(far, "kk", [(r, (r + 2) % zs) for r in range(zs)])
        near_other = lax.ppermute(near, "g", [(1, 0), (3, 2)])
        for x in mine:
            sent.append(lax.ppermute(x, "g", [(2, 1)]))
        out = own_call(zpos1, same, low, up, far, far_other, rows)
        out = slots_call(pos1, out, near, near_other, mine, sent)
        return out[None]

    def step(a):
        return jax.shard_map(local_fn, mesh=mesh, in_specs=(P(("m", "g"), "kk"),), out_specs=P(("m", "g"), None, "kk", None), check_vma=False)(a)

    return step
```

```python
import jax
import jax.numpy as jnp
from jax import lax
from jax.experimental import pallas as pl
from jax.experimental.pallas import tpu as pltpu
from jax.sharding import PartitionSpec as P


PIECES = ((1, 3), (2,), (1,), (1,))
CHIP_SWAP = [(0, 1), (1, 0), (2, 3), (3, 2)]
CROSS = [(0, 3), (1, 2), (2, 0), (3, 1)]
DEPTH = 3584
VMEM = 60 * 1024 * 1024
ANY = pl.BlockSpec(memory_space=pl.ANY)


def dot_t(left, right):
    return lax.dot_general(left, right, (((1,), (1,)), ((), ())), preferred_element_type=jnp.float32)


def mm(load_l, load_r, cols, acc):
    acc[...] = jnp.zeros_like(acc)

    def step(k, _):
        ks = pl.ds(pl.multiple_of(k * DEPTH, DEPTH), DEPTH)
        acc[...] += dot_t(load_l(ks), load_r(ks))
        return 0

    lax.fori_loop(0, cols // DEPTH, step, 0)


def cost(m, n, k):
    return pl.CostEstimate(flops=2 * m * n * k, bytes_accessed=2 * (m + n) * k + 4 * m * n, transcendentals=0)


def params(n):
    return pltpu.CompilerParams(vmem_limit_bytes=VMEM, dimension_semantics=("arbitrary",) * n)


def same_call(a, zs):
    rows, cols = a.shape
    q = rows // zs
    h, e = q // 2, q // 4
    wide = 10 * e

    def body(a_ref, o_ref, left, right):
        mm(lambda ks: a_ref[:, ks], lambda ks: a_ref[:h, ks], cols, left)
        mm(lambda ks: a_ref[h:, ks], lambda ks: a_ref[h:, ks], cols, right)
        o_ref[0, :, :e] = left[:e, :e]
        o_ref[0, :, e : 3 * e] = left[e : 2 * e, :]
        o_ref[0, :, 3 * e : 5 * e] = left[2 * e : 3 * e, :]
        o_ref[0, :, 5 * e : 6 * e] = right[:e, :e]
        o_ref[0, :, 6 * e : 8 * e] = left[3 * e :, :]
        o_ref[0, :, 8 * e :] = right[e:, :]

    return pl.pallas_call(
        body,
        grid=(zs,),
        in_specs=[pl.BlockSpec((q, cols), lambda r: (r, 0))],
        out_specs=pl.BlockSpec((1, e, wide), lambda r: (r, 0, 0)),
        out_shape=jax.ShapeDtypeStruct((zs, e, wide), jnp.float32),
        scratch_shapes=[pltpu.VMEM((q, h), jnp.float32), pltpu.VMEM((h, h), jnp.float32)],
        compiler_params=params(1),
        cost_estimate=cost(rows, q, cols),
        name="same_block",
    )(a)


def rest_call(a, dep, zs):
    rows, cols = a.shape
    q = rows // zs
    h = q // 2

    def body(l_ref, r_ref, dep_ref, o_ref):
        mm(lambda ks: l_ref[:, ks], lambda ks: r_ref[:, ks], cols, o_ref.at[0])

    def left(r, c):
        return (jnp.where((c == 2) & (r >= 2), r - 2, r), 0)

    def right(r, c):
        far = jnp.where(r < 2, 2 * (r + 2), 2 * r + 1)
        return (jnp.where(c == 2, far, 2 * ((r + 3) % 4) + c), 0)

    return pl.pallas_call(
        body,
        grid=(zs, 3),
        in_specs=[pl.BlockSpec((q, cols), left), pl.BlockSpec((h, cols), right), ANY],
        out_specs=pl.BlockSpec((1, q, h), lambda r, c: (r, 0, c)),
        out_shape=jax.ShapeDtypeStruct((zs, q, 3 * h), jnp.float32),
        compiler_params=params(2),
        cost_estimate=cost(rows, 3 * h, cols),
        name="rest_block",
    )(a, a, dep)


def near_call(left, right, which, dep, zs):
    rows, cols = left.shape
    h = rows // zs // 2

    def body(l_ref, r_ref, dep_ref, o_ref):
        mm(lambda ks: l_ref[:, 0, :, ks].reshape(zs * h, -1), lambda ks: r_ref[:, ks], cols, o_ref)

    return pl.pallas_call(
        body,
        grid=(rows // h,),
        in_specs=[
            pl.BlockSpec((zs, 1, h, cols), lambda j: (0, which, 0, 0), pipeline_mode=pl.Buffered(1)),
            pl.BlockSpec((h, cols), lambda j: (j, 0)),
            ANY,
        ],
        out_specs=pl.BlockSpec((zs * h, h), lambda j: (0, j)),
        out_shape=jax.ShapeDtypeStruct((zs * h, rows), jnp.float32),
        compiler_params=params(1),
        cost_estimate=cost(zs * h, rows, cols),
        name="near_block",
    )(left.reshape(zs, 2, h, cols), right, dep)


def cross_call(pos, gots, a, dep, zs):
    rows, cols = a.shape
    q = rows // zs
    sizes = [x.shape[0] // zs for x in gots]
    n = sum(sizes)

    def body(pos_ref, *refs):
        l_refs, (r_ref, dep_ref, o_ref, acc) = refs[: len(sizes)], refs[len(sizes) :]
        j = pl.program_id(0)
        lo = 0
        for l_ref, size in zip(l_refs, sizes):
            part = acc.at[:, : zs * size]
            mm(lambda ks: r_ref[:, ks], lambda ks: l_ref[:, ks], cols, part)

            @pl.when(pos_ref[0] != 2)
            def _():
                prod = part[...].T
                for s in range(zs):
                    o_ref[s, lo : lo + size, pl.ds(pl.multiple_of(j * q, q), q)] = prod[s * size : (s + 1) * size]

            @pl.when(pos_ref[0] == 2)
            def _():
                prod = part[...].T
                for s in range(zs):
                    o_ref[j, lo : lo + size, s * q : (s + 1) * q] = prod[s * size : (s + 1) * size]

            lo += size

    return pl.pallas_call(
        body,
        grid_spec=pltpu.PrefetchScalarGridSpec(
            num_scalar_prefetch=1,
            grid=(zs,),
            in_specs=[pl.BlockSpec(x.shape, lambda j, p: (0, 0), pipeline_mode=pl.Buffered(1)) for x in gots]
            + [pl.BlockSpec((q, cols), lambda j, p: (j, 0)), ANY],
            out_specs=pl.BlockSpec((zs, n, rows), lambda j, p: (0, 0, 0)),
            scratch_shapes=[pltpu.VMEM((q, zs * max(sizes)), jnp.float32)],
        ),
        out_shape=jax.ShapeDtypeStruct((zs, n, rows), jnp.float32),
        compiler_params=params(1),
        cost_estimate=cost(zs * n, rows, cols),
        name="cross_block",
    )(pos, *gots, a, dep)


def own_call(zpos, same, low, up, far, far_other, rows):
    q = low.shape[0]
    e = q // 4

    def body(z_ref, same_ref, low_ref, up_ref, far_ref, other_ref, o_ref):
        z = z_ref[0]

        def cols(rel):
            return pl.ds(pl.multiple_of(((z + rel) % 4) * q, q), q)

        for i in range(4):
            for j in range(4):
                hi, lo = max(i, j), min(i, j)
                at = hi * (hi + 1) // 2 + lo
                tile = same_ref[:, at * e : (at + 1) * e]
                here = pl.ds(pl.multiple_of(z * q + j * e, e), e)
                o_ref[0, i * e : (i + 1) * e, here] = tile if i >= j else tile.T
        o_ref[0, :, cols(1)] = up_ref[...].T
        o_ref[0, :, cols(3)] = low_ref[...]

        @pl.when(z < 2)
        def _():
            o_ref[0, :, cols(2)] = jnp.concatenate([far_ref[...], other_ref[...]], axis=1)

        @pl.when(z >= 2)
        def _():
            o_ref[0, :, cols(2)] = jnp.concatenate([other_ref[...], far_ref[...]], axis=1).T

    whole = lambda x: pl.BlockSpec(x.shape, lambda i, z: (0, 0))
    ins = (same, low, up, far, far_other)
    return pl.pallas_call(
        body,
        grid_spec=pltpu.PrefetchScalarGridSpec(
            num_scalar_prefetch=1,
            grid=(1,),
            in_specs=[whole(x) for x in ins],
            out_specs=pl.BlockSpec((1, q, rows), lambda i, z: (0, 0, 0)),
        ),
        out_shape=jax.ShapeDtypeStruct((3, q, rows), jnp.float32),
        compiler_params=params(1),
        name="own_out",
    )(zpos, *ins)


def slots_call(pos, out, near, near_other, mine, sent):
    _, q, rows = out.shape
    spans = []
    for x in mine:
        lo = spans[-1][1] if spans else 0
        spans.append((lo, lo + x.shape[0]))
    n = len(mine)

    def body(p_ref, out_ref, near_ref, other_ref, *refs):
        mine_refs, sent_refs, o_ref, buf = refs[:n], refs[n : 2 * n], refs[2 * n], refs[2 * n + 1]
        p = p_ref[0]
        slot = pl.program_id(0) + 1

        @pl.when(((slot == 1) & (p == 3)) | ((slot == 2) & (p < 2)))
        def _():
            for (lo, hi), ref in zip(spans, mine_refs):
                o_ref[0, lo:hi, :] = ref[...]

        @pl.when((slot == 2) & (p >= 2))
        def _():
            o_ref[...] = jnp.zeros_like(o_ref)

        @pl.when((slot == 1) & (p % 2 == 0))
        def _():
            o_ref[0, : q // 2, :] = near_ref[...]
            o_ref[0, q // 2 :, :] = other_ref[...]

        @pl.when((slot == 1) & (p == 1))
        def _():
            for (lo, hi), ref in zip(spans, sent_refs):
                buf[lo:hi, :] = ref[...]
            for s in range(rows // q):
                o_ref[0, :, s * q : (s + 1) * q] = buf[:, s * q : (s + 1) * q].T

    whole = lambda x: pl.BlockSpec(x.shape, lambda i, p: (0, 0), pipeline_mode=pl.Buffered(1))
    ins = (near, near_other, *mine, *sent)
    return pl.pallas_call(
        body,
        grid_spec=pltpu.PrefetchScalarGridSpec(
            num_scalar_prefetch=1,
            grid=(2,),
            in_specs=[ANY] + [whole(x) for x in ins],
            out_specs=pl.BlockSpec((1, q, rows), lambda i, p: (i + 1, 0, 0)),
            scratch_shapes=[pltpu.VMEM((q, rows), jnp.float32)],
        ),
        out_shape=jax.ShapeDtypeStruct(out.shape, jnp.float32),
        input_output_aliases={1: 0},
        compiler_params=params(1),
        name="slots_out",
    )(pos, out, *ins)


def solution(mesh):
    assert mesh.shape["g"] == 4 and mesh.shape["kk"] == 4
    zs = 4

    def scatter(parts):
        return lax.psum_scatter(parts, "kk", scatter_dimension=0, tiled=False)

    def local_fn(a):
        pos = lax.axis_index("g").astype(jnp.int32)
        zpos = lax.axis_index("kk").astype(jnp.int32)
        pos1, zpos1 = pos.reshape(1), zpos.reshape(1)
        rows, cols = a.shape
        q = rows // zs
        h = q // 2
        a4 = a.reshape(zs, q, cols)
        unit = q // sum(map(sum, PIECES))

        arrived, start, gives = [], 0, 0
        for sizes in PIECES:
            arrived.append([])
            for n in sizes:
                piece = a4[:, start : start + n * unit].reshape(-1, cols)
                arrived[-1].append(lax.ppermute(piece, "g", CROSS))
                start += n * unit
                gives += 1
        partner = lax.ppermute(a, "g", CHIP_SWAP)

        same_part = same_call(a, zs)
        same = scatter(same_part)
        rest_part = rest_call(a, same_part, zs)
        rest = scatter(rest_part)

        even = pos % 2 == 0
        near_part = lax.cond(
            even,
            lambda: near_call(partner, a, 0, rest_part, zs),
            lambda: near_call(a, partner, 1, rest_part, zs),
        )
        near = scatter(near_part.reshape(zs, h, rows))

        mine, sent, dep = [], [], near_part
        for got in arrived:
            dep = cross_call(pos1, got, a, dep, zs)
            mine.append(scatter(dep))

        low, far = rest[:, :q], rest[:, q:]
        up = lax.ppermute(low, "kk", [(r, (r - 1) % zs) for r in range(zs)])
        far_other = lax.ppermute(far, "kk", [(r, (r + 2) % zs) for r in range(zs)])
        near_other = lax.ppermute(near, "g", [(1, 0), (3, 2)])
        for x in mine:
            sent.append(lax.ppermute(x, "g", [(2, 1)]))
        out = own_call(zpos1, same, low, up, far, far_other, rows)
        out = slots_call(pos1, out, near, near_other, mine, sent)
        return out[None]

    def step(a):
        return jax.shard_map(local_fn, mesh=mesh, in_specs=(P(("m", "g"), "kk"),), out_specs=P(("m", "g"), None, "kk", None), check_vma=False)(a)

    return step
```
